512 devices in a mesh: dp: 32 (over x_lo, y, core), slab: 16 (over x_hi, z).
Axes of the slice: x: 4 (x_hi: 2, x_lo: 2; x = x_hi * 2 + x_lo), y: 8, z: 8, core: 2. Of those that a mesh axis runs over, the one named last changes fastest.
Arguments:
- activation: bfloat16 [128, 64, 128, 256], P('dp', None, 'slab'), may hold values from -6 to 6
- cotangent: bfloat16 [128, 64, 128, 256], P('dp', None, 'slab'), may hold values from -6 to 6
- spectral_weight: bfloat16 [64, 32, 32, 128], P(None, 'slab'), may hold values from -0.75 to 0.75
Outputs:
- input_grad: bfloat16 [128, 64, 128, 256], P('dp', None, 'slab')
- weight_grad: float32 [64, 32, 32, 128], P('dp', 'slab')
The draws below stay inside these ranges and needn't reach their ends.
All inputs are finite; a program needn't handle non-finite values.
Results may differ from the reference program's by a relative error of at most 0.023.
Values may be sent and summed in bfloat16 or wider, within the bound.
A program may use at most 64 MiB of HBM per device.

```python
import math
import jax
import jax.numpy as jnp

C = 64
X = 128
Y = 128
MX = 32
MY = 32
BATCH = 128


def strengthened(values, own_key, source, target, shards_of, factor):
    owner, partner = [(jnp.arange(values.shape[position]) // (values.shape[position] // shards_of)).reshape([-1 if axis == position else 1 for axis in range(values.ndim)]) for position in (source, target)]
    chosen = jax.random.permutation(own_key, shards_of)[partner]
    strong = (owner == chosen) | (owner == (partner + shards_of // 2) % shards_of)
    return jnp.where(strong, factor * values, values)


def steps_of(own_key, extent, shards, smallest, largest):
    def one(dim, shards_of):
        steps = jax.random.uniform(jax.random.fold_in(jax.random.fold_in(own_key, 6), dim), (shards_of,), jnp.float32, smallest / len(shards), largest / len(shards))
        return jnp.repeat(jnp.exp(steps), extent[dim] // shards_of).reshape((-1,) + (1,) * (len(extent) - dim - 1))

    loudness = one(*shards[0])
    for cut in shards[1:]:
        loudness = loudness * one(*cut)
    return loudness


def centred(rng, extent, scale, bound, cuts=(), held_as=jnp.bfloat16):
    loudness = steps_of(rng, extent, cuts, -0.22, 0.18) if cuts else 1.0
    entries = jax.random.normal(rng, extent, jnp.float32) * scale * loudness
    return jnp.minimum(jnp.maximum(entries, -bound), bound).astype(held_as)


def bell_draw_with(own_key, shape, scale, bound, pieces, heavy, kind=jnp.bfloat16):
    array = scale * jax.random.normal(own_key, shape, jnp.float32)
    if pieces:
        array = array * steps_of(own_key, shape, pieces, -0.22, 0.18)
    return jnp.clip(strengthened(array, jax.random.fold_in(own_key, 3), *heavy), -bound, bound).astype(kind)


def setup_inputs(seed: int = 0) -> dict:
    splits = jax.random.split(jax.random.key(seed), 4)
    return {
        "activation": bell_draw_with(splits[0], (BATCH, C, X, 2 * Y), 1.0, 6.0, ((0, 32), (2, 16)), (0, 1, 32, 2.75)),
        "cotangent": centred(splits[1], (BATCH, C, X, 2 * Y), 1.0, 6.0, ((0, 32), (2, 16))),
        "spectral_weight": centred(splits[2], (C, MY, MX, 2 * C), C ** -0.5, 0.75, ((1, 16),)),
    }


def retained(length, modes):
    index = jnp.arange(modes, dtype=jnp.int32)
    return jnp.where(index < modes // 2, index, index + (length - modes))

def cos_sin(length, modes):
    cells = jnp.arange(length, dtype=jnp.int32)
    phase = cells[:, None] * retained(length, modes)[None, :] % length
    angle = phase.astype(jnp.float32) * (2.0 * math.pi / length)
    factor = 1.0 / math.sqrt(length)
    return ((jnp.cos(angle) * factor).astype(jnp.bfloat16), (jnp.sin(angle) * factor).astype(jnp.bfloat16))

def y_table(cosine_table, sine_table):
    upper = jnp.concatenate([cosine_table, -sine_table], axis=1)
    lower = jnp.concatenate([sine_table, cosine_table], axis=1)
    return jnp.concatenate([upper, lower], axis=0)

def x_table(cosine_table, sine_table):
    first = jnp.stack([cosine_table, -sine_table], axis=2)
    second = jnp.stack([sine_table, cosine_table], axis=2)
    return jnp.stack([first, second], axis=1)

def reference(activation, cotangent, spectral_weight):
    cos_y, sin_y = cos_sin(Y, MY)
    cos_x, sin_x = cos_sin(X, MX)
    table_y = y_table(cos_y, sin_y)
    table_x = x_table(cos_x, sin_x).astype(jnp.float32)

    def spectrum(volume):
        lines = volume.reshape(-1, 2 * Y)
        along = jnp.dot(lines, table_y, preferred_element_type=jnp.float32).astype(jnp.bfloat16)
        along = along.reshape(BATCH, C, X, 2, MY).astype(jnp.float32)
        return jnp.einsum('bcxpt,xpkq->bckqt', along, table_x).astype(jnp.bfloat16)
    spec_in = spectrum(activation).astype(jnp.float32)
    spec_out = spectrum(cotangent).astype(jnp.float32)
    swapped = jnp.stack([spec_out[:, :, :, 1], -spec_out[:, :, :, 0]], axis=3)
    real_part = jnp.einsum('bikpt,bokpt->itko', spec_in, spec_out)
    imag_part = jnp.einsum('bikpt,bokpt->itko', spec_in, swapped)
    weight_grad = jnp.stack([real_part, imag_part], axis=3).reshape(C, MY, MX, 2 * C)
    weight = spectral_weight.astype(jnp.float32).reshape(C, MY, MX, 2, C)
    grad_real = jnp.einsum('bokpt,itkpo->bikt', spec_out, weight)
    grad_imag = jnp.einsum('bokpt,itkpo->bikt', swapped, weight)
    spec_grad = jnp.stack([grad_real, grad_imag], axis=3).astype(jnp.bfloat16).astype(jnp.float32)
    spread = jnp.einsum('bikqt,xpkq->bixpt', spec_grad, table_x).astype(jnp.bfloat16)
    lines = spread.reshape(-1, 2 * MY)
    values = jnp.dot(lines, table_y.T, preferred_element_type=jnp.float32).astype(jnp.bfloat16)
    input_grad = values.reshape(BATCH, C, X, 2 * Y)
    return (input_grad, weight_grad)
```

```python
import functools

import jax
import jax.numpy as jnp
import numpy as np
from jax import lax
from jax.experimental import pallas as pl
from jax.experimental.pallas import tpu as pltpu
from jax.sharding import PartitionSpec as P

MESH = pl.DeviceIdType.MESH
F32 = jnp.float32
BF16 = jnp.bfloat16


def retained(length, modes):
    index = np.arange(modes)
    return np.where(index < modes // 2, index, index + (length - modes))


def cos_sin(length, modes):
    phase = np.arange(length)[:, None] * retained(length, modes)[None, :] % length
    angle = phase * (2.0 * np.pi / length)
    factor = 1.0 / np.sqrt(length)
    return np.cos(angle) * factor, np.sin(angle) * factor


def tables(slabs):
    cos_y, sin_y = cos_sin(128, 32)
    table_y = np.concatenate(
        [np.concatenate([cos_y, -sin_y], 1), np.concatenate([sin_y, cos_y], 1)], 0
    )
    ty = table_y.reshape(256, 2, slabs, 32 // slabs).transpose(2, 3, 1, 0).reshape(64, 256)
    cos_x, sin_x = cos_sin(128, 32)
    table_x = np.stack(
        [np.stack([cos_x, -sin_x], 2), np.stack([sin_x, cos_x], 2)], 1
    )
    fx = table_x.reshape(slabs, 128 // slabs, 2, 32, 2).transpose(4, 3, 0, 2, 1).reshape(64, 256)
    return jnp.asarray(ty, BF16), jnp.asarray(fx, BF16), jnp.asarray(fx.T.copy(), BF16)


def ring(step):
    return 4 + (1 - 2 * lax.rem(step, 2)) * lax.div(step + 1, 2)


def slab_peer(me, step):
    across = lax.rem(lax.div(me, 8) + 1 - lax.rem(step, 2), 2)
    return across * 8 + lax.rem(lax.rem(me, 8) + ring(lax.div(step, 2)), 8)


def dp_peer(me, step):
    sub = lax.rem(step, 4)
    core = lax.rem(lax.rem(me, 2) + 1 - lax.rem(sub, 2), 2)
    across = lax.rem(lax.div(me, 16) + 1 - lax.div(sub, 2), 2)
    along = lax.rem(lax.rem(lax.div(me, 2), 8) + ring(lax.div(step, 4)), 8)
    return (across * 8 + along) * 2 + core


def nt(a, b):
    return lax.dot_general(a, b, (((1,), (1,)), ((), ())), preferred_element_type=F32)


def tn(a, b):
    return lax.dot_general(a, b, (((0,), (0,)), ((), ())), preferred_element_type=F32)


def kernel(
    slabs, groups,
    act_hbm, cot_hbm, w_hbm, ty_ref, fx_ref, tx_ref,
    grad_ref, wgrad_ref,
    act_v, cot_v, w_v, wm, lines, folded,
    send_a, send_c, got_a, got_c, send_e, got_e,
    spectra, pair_a, pair_c, all_a, all_c, stacked, mixed, sums, wsend,
    load_sem, send_sem, recv_sem,
):
    me_s = lax.axis_index("slab")
    me_d = lax.axis_index("dp")

    loads = [
        pltpu.make_async_copy(src, dst, load_sem.at[n])
        for n, (src, dst) in enumerate(((cot_hbm, cot_v), (act_hbm, act_v), (w_hbm, w_v)))
    ]
    for load in loads:
        load.start()

    barrier = pltpu.get_barrier_semaphore()

    @pl.loop(0, slabs - 1)
    def _(step):
        pl.semaphore_signal(
            barrier, inc=1, device_id={"slab": slab_peer(me_s, step)}, device_id_type=MESH
        )

    @pl.loop(0, groups - 1)
    def _(step):
        pl.semaphore_signal(
            barrier, inc=1, device_id={"dp": dp_peer(me_d, step)}, device_id_type=MESH
        )

    def exchange(axis, me, peer_of, count, src, dst, n):
        @pl.loop(0, count - 1)
        def _(step):
            peer = peer_of(me, step)
            pltpu.make_async_remote_copy(
                src_ref=src.at[peer], dst_ref=dst.at[me], send_sem=send_sem.at[n],
                recv_sem=recv_sem.at[n], device_id={axis: peer}, device_id_type=MESH,
            ).start()

    def wait_all(ref, count, sem):
        part = ref.at[pl.ds(0, count - 1)]
        pltpu.make_async_copy(part, part, sem).wait()

    over_slab = functools.partial(exchange, "slab", me_s, slab_peer, slabs)
    over_dp = functools.partial(exchange, "dp", me_d, dp_peer, groups)

    def along_y(field, send):
        for c in range(8):
            part = field[c * 32 : (c + 1) * 32].astype(F32).reshape(256, 256)
            for half in range(2):
                lines[half, c * 256 : (c + 1) * 256, :] = part[:, half * 128 : half * 128 + 128]
        for r in range(8):
            rows = jnp.concatenate(
                [lines[half, pl.ds(r, 256, stride=8), :] for half in range(2)], axis=1
            ).astype(BF16)
            moved = nt(ty_ref[...], rows)
            for half in range(2):
                folded[half, pl.ds(r, 64, stride=8), :] = moved[:, half * 128 : half * 128 + 128]
        for half in range(2):
            send[:, :, :, half * 128 : half * 128 + 128] = (
                folded[half].astype(BF16).reshape(slabs, 2, 16, 128)
            )

    loads[0].wait()
    along_y(cot_v, send_c)
    got_c[me_s] = send_c[me_s]
    pl.semaphore_wait(barrier, slabs + groups - 2)
    over_slab(send_c, got_c, 0)
    loads[1].wait()
    along_y(act_v, send_a)
    got_a[me_s] = send_a[me_s]
    over_slab(send_a, got_a, 1)

    loads[2].wait()
    for c in range(8):
        part = w_v[c * 8 : (c + 1) * 8].astype(F32).reshape(512, 128)
        lines[c // 4, c % 4 * 512 : (c % 4 + 1) * 512, :] = part

    @pl.loop(0, 64)
    def _(m):
        for half in range(2):
            wm[m, half * 32 : half * 32 + 32, :] = lines[
                half, pl.ds(m, 32, stride=64), :
            ].astype(BF16)

    lane = lax.broadcasted_iota(jnp.int32, (32, 128), 1)
    low = lane < 64

    def spec_of(got):
        return [
            jnp.dot(fx_ref[...], got[:, t].reshape(256, 256), preferred_element_type=F32)
            .astype(BF16)
            .astype(F32)
            for t in range(2)
        ]

    def to_pair(specs, pair):
        for t in range(2):
            for q in range(2):
                for h in range(2):
                    spectra[pl.ds(t * 128 + q * 2 + h, 32, stride=4), :] = specs[t][
                        q * 32 : q * 32 + 32, h * 128 : h * 128 + 128
                    ]
        pair[...] = spectra[...].astype(BF16).reshape(groups, 256 // groups, 128)

    wait_all(got_c, slabs, recv_sem.at[0])
    specs = spec_of(got_c)

    for t in range(2):
        for h in range(2):
            re = specs[t][0:32, h * 128 : h * 128 + 128]
            im = specs[t][32:64, h * 128 : h * 128 + 128]
            re_r = pltpu.roll(re, 64, 1)
            im_r = pltpu.roll(im, 64, 1)
            rows = (
                jnp.where(low, re, im_r),
                jnp.where(low, im, -re_r),
                jnp.where(low, re_r, im),
                jnp.where(low, im_r, -re),
            )
            for n, row in enumerate(rows):
                stacked[pl.ds(t * 256 + h * 4 + n, 32, stride=8), :] = row

    @pl.loop(0, 32)
    def _(n):
        both = nt(
            stacked[pl.ds(pl.multiple_of(n * 16, 16), 16), :].astype(BF16),
            wm[pl.ds(n * 2, 2)].reshape(128, 128),
        )
        turned = pltpu.roll(both, 64, 1)
        mixed[pl.ds(pl.multiple_of(n * 16, 16), 8), :] = both[0:8]
        mixed[pl.ds(pl.multiple_of(n * 16 + 8, 8), 8), :] = turned[8:16]

    for t in range(2):
        rows = []
        for q in range(2):
            tiles = []
            for h in range(2):
                first = mixed[pl.ds(t * 256 + h * 4 + q, 32, stride=8), :]
                second = mixed[pl.ds(t * 256 + h * 4 + 2 + q, 32, stride=8), :]
                tiles.append(jnp.where(low, first, pltpu.roll(second, 64, 1)))
            rows.append(jnp.concatenate(tiles, axis=1))
        grads = jnp.concatenate(rows, axis=0).astype(BF16)
        spread = jnp.dot(tx_ref[...], grads, preferred_element_type=F32)
        send_e[:, t] = spread.astype(BF16).reshape(slabs, 16, 256)
    got_e[me_s] = send_e[me_s]
    over_slab(send_e, got_e, 2)

    to_pair(specs, pair_c)
    all_c[me_d] = pair_c[me_d]
    over_dp(pair_c, all_c, 3)

    wait_all(got_a, slabs, recv_sem.at[1])
    to_pair(spec_of(got_a), pair_a)
    all_a[me_d] = pair_a[me_d]
    over_dp(pair_a, all_a, 4)

    wait_all(all_c, groups, recv_sem.at[3])
    wait_all(all_a, groups, recv_sem.at[4])
    sums[0] = all_a[...].astype(F32).reshape(256, 128)
    sums[1] = all_c[...].astype(F32).reshape(256, 128)
    wide = lax.broadcasted_iota(jnp.int32, (64, 128), 1) < 64
    for m in range(2):
        def part(which, q):
            return jnp.concatenate(
                [sums[which, pl.ds(m * 4 + q * 2 + h, groups, stride=8), :] for h in range(2)],
                axis=0,
            )

        ins = jnp.concatenate([part(0, 0), part(0, 1)], axis=0).astype(BF16)
        out_re, out_im = part(1, 0), part(1, 1)
        outs = jnp.concatenate([out_re, out_im], axis=0)
        swapped = jnp.concatenate([out_im, -out_re], axis=0)
        prod = tn(ins, jnp.concatenate([outs, swapped], axis=1).astype(BF16))
        top, bottom = prod[0:64], prod[64:128]
        total = jnp.where(
            wide,
            top[:, 0:128] + pltpu.roll(bottom[:, 0:128], 64, 1),
            pltpu.roll(top[:, 128:256], 64, 1) + bottom[:, 128:256],
        )
        mixed[m * 64 : m * 64 + 64, :] = total
    for m in range(2):
        for i in range(2):
            wsend[:, i, m, :] = mixed[pl.ds(m * 64 + i, groups, stride=2), :]
    wgrad_ref[me_d] = wsend[me_d]
    over_dp(wsend, wgrad_ref, 5)

    wait_all(got_e, slabs, recv_sem.at[2])
    for half in range(2):
        folded[half] = got_e[:, :, :, half * 128 : half * 128 + 128].astype(F32).reshape(512, 128)
    for r in range(8):
        rows = jnp.concatenate(
            [folded[half, pl.ds(r, 64, stride=8), :] for half in range(2)], axis=1
        ).astype(BF16)
        values = tn(rows, ty_ref[...])
        for half in range(2):
            lines[half, pl.ds(r, 256, stride=8), :] = values[:, half * 128 : half * 128 + 128]
    for c in range(8):
        grad_ref[c * 32 : (c + 1) * 32] = (
            jnp.concatenate(
                [lines[half, c * 256 : (c + 1) * 256, :] for half in range(2)], axis=1
            )
            .astype(BF16)
            .reshape(32, 8, 256)
        )

    wait_all(wgrad_ref, groups, recv_sem.at[5])
    for n, ref in enumerate((send_c, send_a, send_e)):
        wait_all(ref, slabs, send_sem.at[n])
    for n, ref in enumerate((pair_c, pair_a, wsend)):
        wait_all(ref, groups, send_sem.at[3 + n])


def body(activation, cotangent, spectral_weight, slabs, groups):
    ty, fx, tx = tables(slabs)
    vmem = pl.BlockSpec(memory_space=pltpu.VMEM)
    hbm = pl.BlockSpec(memory_space=pl.ANY)
    block = (slabs, 2, 16, 256)
    pair = (groups, 256 // groups, 128)
    grad, wgrad = pl.pallas_call(
        functools.partial(kernel, slabs, groups),
        out_shape=(
            jax.ShapeDtypeStruct((256, 8, 256), BF16),
            jax.ShapeDtypeStruct((groups, 2, 2, 128), F32),
        ),
        in_specs=[hbm] * 3 + [vmem] * 3,
        out_specs=[vmem, vmem],
        scratch_shapes=[
            pltpu.VMEM((256, 8, 256), BF16),
            pltpu.VMEM((256, 8, 256), BF16),
            pltpu.VMEM((64, 64, 128), BF16),
            pltpu.VMEM((64, 64, 128), BF16),
            pltpu.VMEM((2, 2048, 128), F32),
            pltpu.VMEM((2, 512, 128), F32),
        ]
        + [pltpu.VMEM(block, BF16)] * 6
        + [pltpu.VMEM((256, 128), F32)]
        + [pltpu.VMEM(pair, BF16)] * 4
        + [
            pltpu.VMEM((512, 128), F32),
            pltpu.VMEM((512, 128), F32),
            pltpu.VMEM((2, 256, 128), F32),
            pltpu.VMEM((groups, 2, 2, 128), F32),
            pltpu.SemaphoreType.DMA((3,)),
            pltpu.SemaphoreType.DMA((6,)),
            pltpu.SemaphoreType.DMA((6,)),
        ],
        compiler_params=pltpu.CompilerParams(collective_id=0, has_side_effects=True),
    )(
        activation.reshape(256, 8, 256),
        cotangent.reshape(256, 8, 256),
        spectral_weight.reshape(64, 64, 128),
        ty,
        fx,
        tx,
    )
    wgrad = wgrad.transpose(1, 0, 2, 3).reshape(2, 2, 32, 128)
    return grad.reshape(4, 64, 8, 256), wgrad


def solution(mesh):
    placed = (P("dp", None, "slab", None), P("dp", None, "slab", None), P(None, "slab", None, None))
    return jax.shard_map(
        functools.partial(body, slabs=mesh.shape["slab"], groups=mesh.shape["dp"]),
        mesh=mesh,
        in_specs=placed,
        out_specs=(P("dp", None, "slab", None), P("dp", "slab", None, None)),
        check_vma=False,
    )
```

```python
import functools

import jax
import jax.numpy as jnp
import numpy as np
from jax import lax
from jax.experimental import pallas as pl
from jax.experimental.pallas import tpu as pltpu
from jax.sharding import PartitionSpec as P

MESH = pl.DeviceIdType.MESH
F32 = jnp.float32
BF16 = jnp.bfloat16


def retained(length, modes):
    index = np.arange(modes)
    return np.where(index < modes // 2, index, index + (length - modes))


def cos_sin(length, modes):
    phase = np.arange(length)[:, None] * retained(length, modes)[None, :] % length
    angle = phase * (2.0 * np.pi / length)
    factor = 1.0 / np.sqrt(length)
    return np.cos(angle) * factor, np.sin(angle) * factor


def tables(slabs):
    cos_y, sin_y = cos_sin(128, 32)
    table_y = np.concatenate(
        [np.concatenate([cos_y, -sin_y], 1), np.concatenate([sin_y, cos_y], 1)], 0
    )
    ty = table_y.reshape(256, 2, slabs, 32 // slabs).transpose(2, 3, 1, 0).reshape(64, 256)
    cos_x, sin_x = cos_sin(128, 32)
    table_x = np.stack(
        [np.stack([cos_x, -sin_x], 2), np.stack([sin_x, cos_x], 2)], 1
    )
    fx = table_x.reshape(slabs, 128 // slabs, 2, 32, 2).transpose(4, 3, 0, 2, 1).reshape(64, 256)
    packed = np.zeros((2048, 256), np.float32)
    packed[0:64], packed[64:128], packed[128:384, 0:64] = ty, fx, fx.T
    return jnp.asarray(ty, BF16), jnp.asarray(packed, BF16)


RING = (4, 3, 5, 2, 6, 1, 7, 0)


def slab_peers(me):
    part, along = lax.div(me, 8), lax.rem(me, 8)
    parts = [lax.rem(part + n, 2) * 8 for n in range(2)]
    peers = [parts[n] + lax.rem(along + off, 8) for off in RING for n in (1, 0)]
    return peers[:-1]


def dp_peers(me):
    part, along, core = lax.div(me, 16), lax.rem(lax.div(me, 2), 8), lax.rem(me, 2)
    parts = [lax.rem(part + n, 2) * 16 for n in range(2)]
    cores = [lax.rem(core + n, 2) for n in range(2)]
    peers = []
    for off in RING:
        row = lax.rem(along + off, 8) * 2
        peers += [row + parts[n] + cores[c] for n in (1, 0) for c in (1, 0)]
    return peers[:-1]


def nt(a, b):
    return lax.dot_general(a, b, (((1,), (1,)), ((), ())), preferred_element_type=F32)


def tn(a, b):
    return lax.dot_general(a, b, (((0,), (0,)), ((), ())), preferred_element_type=F32)


def kernel(
    slabs, groups,
    act_hbm, cot_hbm, w_hbm, tab_hbm,
    got_e, wgrad_ref,
    ty_ref, fx_ref, tx_ref, act_v, cot_v, w_v, wm, lines, folded,
    send_a, send_c, got_a, got_c, send_e,
    spectra, pair_a, pair_c, all_a, all_c, stacked, mixed, sums, wsend,
    load_sem, send_sem, recv_sem,
):
    me_s = lax.axis_index("slab")
    me_d = lax.axis_index("dp")

    loads = [
        pltpu.make_async_copy(src, dst, load_sem.at[n])
        for n, (src, dst) in enumerate(
            (
                (tab_hbm.at[pl.ds(0, 64)], ty_ref),
                (cot_hbm.at[pl.ds(0, 128)], cot_v.at[pl.ds(0, 128)]),
                (cot_hbm.at[pl.ds(128, 128)], cot_v.at[pl.ds(128, 128)]),
                (act_hbm, act_v), (w_hbm, w_v),
                (tab_hbm.at[pl.ds(64, 64)], fx_ref),
                (tab_hbm.at[pl.ds(128, 256), pl.ds(0, 128)], tx_ref),
            )
        )
    ]
    for load in loads:
        load.start()

    peers_s, peers_d = slab_peers(me_s), dp_peers(me_d)
    barrier = pltpu.get_barrier_semaphore()
    for axis, peers in (("slab", peers_s), ("dp", peers_d)):
        for peer in peers:
            pl.semaphore_signal(barrier, inc=1, device_id={axis: peer}, device_id_type=MESH)

    def exchange(axis, me, peers, src, dst, n, rank=0):
        lead = (slice(None),) * rank
        for peer in peers:
            pltpu.make_async_remote_copy(
                src_ref=src.at[(*lead, peer)], dst_ref=dst.at[(*lead, me)],
                send_sem=send_sem.at[n], recv_sem=recv_sem.at[n],
                device_id={axis: peer}, device_id_type=MESH,
            ).start()

    def wait_all(ref, count, sem):
        part = ref.at[pl.ds(0, count - 1)] if ref.shape[0] == count else ref.at[:, pl.ds(0, count - 1)]
        pltpu.make_async_copy(part, part, sem).wait()

    over_slab = functools.partial(exchange, "slab", me_s, peers_s)
    over_dp = functools.partial(exchange, "dp", me_d, peers_d)

    def along_y(field, send, h):
        for c in range(4):
            part = field[h * 128 + c * 32 : h * 128 + (c + 1) * 32].astype(F32).reshape(256, 256)
            for half in range(2):
                lines[half, c * 256 : (c + 1) * 256, :] = part[:, half * 128 : half * 128 + 128]
        for r in range(8):
            rows = jnp.concatenate(
                [lines[half, pl.ds(r, 128, stride=8), :] for half in range(2)], axis=1
            ).astype(BF16)
            folded[pl.ds(r, 64, stride=8), :] = nt(ty_ref[...], rows)
        send[h] = folded[...].astype(BF16).reshape(slabs, 2, 16, 128)

    loads[0].wait()
    loads[1].wait()
    along_y(cot_v, send_c, 0)
    pl.semaphore_wait(barrier, slabs + groups - 2)
    over_slab(send_c.at[0], got_c.at[0], 0)
    loads[2].wait()
    along_y(cot_v, send_c, 1)
    over_slab(send_c.at[1], got_c.at[1], 1)
    for h in range(2):
        got_c[h, me_s] = send_c[h, me_s]
    loads[3].wait()
    along_y(act_v, send_a, 0)
    along_y(act_v, send_a, 1)
    over_slab(send_a, got_a, 2, rank=1)
    for h in range(2):
        got_a[h, me_s] = send_a[h, me_s]

    loads[4].wait()
    for c in range(8):
        part = w_v[c * 8 : (c + 1) * 8].astype(F32).reshape(512, 128)
        lines[c // 4, c % 4 * 512 : (c % 4 + 1) * 512, :] = part

    @pl.loop(0, 64)
    def _(m):
        for half in range(2):
            wm[m, half * 32 : half * 32 + 32, :] = lines[
                half, pl.ds(m, 32, stride=64), :
            ].astype(BF16)

    lane = lax.broadcasted_iota(jnp.int32, (32, 128), 1)
    low = lane < 64

    def spec_of(got):
        return [
            [
                jnp.dot(fx_ref[...], got[h, :, t].reshape(256, 128), preferred_element_type=F32)
                .astype(BF16)
                .astype(F32)
                for h in range(2)
            ]
            for t in range(2)
        ]

    def to_pair(specs, pair):
        for t in range(2):
            for q in range(2):
                for h in range(2):
                    spectra[pl.ds(t * 128 + q * 2 + h, 32, stride=4), :] = specs[t][h][
                        q * 32 : q * 32 + 32
                    ]
        pair[...] = spectra[...].astype(BF16).reshape(groups, 256 // groups, 128)

    wait_all(got_c.at[0], slabs, recv_sem.at[0])
    wait_all(got_c.at[1], slabs, recv_sem.at[1])
    loads[5].wait()
    loads[6].wait()
    specs = spec_of(got_c)

    for t in range(2):
        for h in range(2):
            re, im = specs[t][h][0:32], specs[t][h][32:64]
            re_r = pltpu.roll(re, 64, 1)
            im_r = pltpu.roll(im, 64, 1)
            rows = (
                jnp.where(low, re, im_r),
                jnp.where(low, im, -re_r),
                jnp.where(low, re_r, im),
                jnp.where(low, im_r, -re),
            )
            for n, row in enumerate(rows):
                stacked[pl.ds(t * 256 + h * 4 + n, 32, stride=8), :] = row

    for n in range(16):
        both = nt(
            stacked[n * 32 : n * 32 + 32, :].astype(BF16),
            wm[n * 4 : n * 4 + 4].reshape(256, 128),
        )
        for m in range(4):
            block = both[m * 8 : m * 8 + 8, m // 2 * 128 : m // 2 * 128 + 128]
            mixed[n * 32 + m * 8 : n * 32 + m * 8 + 8, :] = (
                pltpu.roll(block, 64, 1) if m % 2 else block
            )

    for t in range(2):
        rows = []
        for q in range(2):
            tiles = []
            for h in range(2):
                first = mixed[pl.ds(t * 256 + h * 4 + q, 32, stride=8), :]
                second = mixed[pl.ds(t * 256 + h * 4 + 2 + q, 32, stride=8), :]
                tiles.append(jnp.where(low, first, pltpu.roll(second, 64, 1)))
            rows.append(jnp.concatenate(tiles, axis=1))
        grads = jnp.concatenate(rows, axis=0).astype(BF16)
        spread = jnp.dot(tx_ref[:, 0:64], grads, preferred_element_type=F32)
        for h in range(2):
            send_e[h, :, t] = (
                spread[:, h * 128 : h * 128 + 128].astype(BF16).reshape(slabs, 16, 128)
            )
    for h in range(2):
        got_e[h, me_s] = send_e[h, me_s]
    over_slab(send_e, got_e, 3, rank=1)

    to_pair(specs, pair_c)
    all_c[me_d] = pair_c[me_d]
    over_dp(pair_c, all_c, 4)

    wait_all(got_a, slabs, recv_sem.at[2])
    to_pair(spec_of(got_a), pair_a)
    all_a[me_d] = pair_a[me_d]
    over_dp(pair_a, all_a, 5)

    wait_all(all_c, groups, recv_sem.at[4])
    wait_all(all_a, groups, recv_sem.at[5])
    sums[0] = all_a[...].astype(F32).reshape(256, 128)
    sums[1] = all_c[...].astype(F32).reshape(256, 128)
    wide = lax.broadcasted_iota(jnp.int32, (64, 128), 1) < 64
    for m in range(2):
        def part(which, q):
            return jnp.concatenate(
                [sums[which, pl.ds(m * 4 + q * 2 + h, groups, stride=8), :] for h in range(2)],
                axis=0,
            )

        ins = jnp.concatenate([part(0, 0), part(0, 1)], axis=0).astype(BF16)
        out_re, out_im = part(1, 0), part(1, 1)
        outs = jnp.concatenate([out_re, out_im], axis=0)
        swapped = jnp.concatenate([out_im, -out_re], axis=0)
        prod = tn(ins, jnp.concatenate([outs, swapped], axis=1).astype(BF16))
        top, bottom = prod[0:64], prod[64:128]
        total = jnp.where(
            wide,
            top[:, 0:128] + pltpu.roll(bottom[:, 0:128], 64, 1),
            pltpu.roll(top[:, 128:256], 64, 1) + bottom[:, 128:256],
        )
        mixed[m * 64 : m * 64 + 64, :] = total
    for m in range(2):
        for i in range(2):
            wsend[i, :, m, :] = mixed[pl.ds(m * 64 + i, groups, stride=2), :]
    for i in range(2):
        wgrad_ref[i, me_d] = wsend[i, me_d]
    over_dp(wsend, wgrad_ref, 6, rank=1)

    wait_all(got_e, slabs, recv_sem.at[3])
    wait_all(wgrad_ref, groups, recv_sem.at[6])
    for n, ref in enumerate((send_c.at[0], send_c.at[1], send_a, send_e)):
        wait_all(ref, slabs, send_sem.at[n])
    for n, ref in enumerate((pair_c, pair_a, wsend)):
        wait_all(ref, groups, send_sem.at[4 + n])


def expand(got_ref, ty_ref, wgrad_ref, grad_hbm, wgrad_hbm, folded, lines, grad_v, sems):
    copies = [pltpu.make_async_copy(wgrad_ref, wgrad_hbm, sems.at[0])]
    copies[0].start()
    for h in range(2):
        folded[h] = got_ref[h].astype(F32).reshape(512, 128)
        for r in range(8):
            values = tn(folded[h, pl.ds(r, 64, stride=8), :].astype(BF16), ty_ref[...])
            for half in range(2):
                lines[h, half, pl.ds(r, 128, stride=8), :] = values[
                    :, half * 128 : half * 128 + 128
                ]
        for c in range(4):
            grad_v[h, c * 32 : (c + 1) * 32] = (
                jnp.concatenate(
                    [lines[h, half, c * 256 : (c + 1) * 256, :] for half in range(2)], axis=1
                )
                .astype(BF16)
                .reshape(32, 8, 256)
            )
        copies.append(
            pltpu.make_async_copy(
                grad_v.at[h], grad_hbm.at[pl.ds(h * 128, 128)], sems.at[h + 1]
            )
        )
        copies[-1].start()
    for copy in copies:
        copy.wait()


def body(activation, cotangent, spectral_weight, slabs, groups):
    ty, packed = tables(slabs)
    block = (2, slabs, 2, 16, 128)
    pair = (groups, 256 // groups, 128)
    total = (2, groups, 2, 128)
    got, wgrad = pl.pallas_call(
        functools.partial(kernel, slabs, groups),
        out_shape=(jax.ShapeDtypeStruct(block, BF16), jax.ShapeDtypeStruct(total, F32)),
        in_specs=[pl.BlockSpec(memory_space=pltpu.HBM)] * 4,
        out_specs=[pl.BlockSpec(memory_space=pltpu.VMEM)] * 2,
        scratch_shapes=[
            pltpu.VMEM((64, 256), BF16),
            pltpu.VMEM((64, 256), BF16),
            pltpu.VMEM((256, 128), BF16),
            pltpu.VMEM((256, 8, 256), BF16),
            pltpu.VMEM((256, 8, 256), BF16),
            pltpu.VMEM((64, 64, 128), BF16),
            pltpu.VMEM((64, 64, 128), BF16),
            pltpu.VMEM((2, 2048, 128), F32),
            pltpu.VMEM((512, 128), F32),
        ]
        + [pltpu.VMEM(block, BF16)] * 5
        + [pltpu.VMEM((256, 128), F32)]
        + [pltpu.VMEM(pair, BF16)] * 4
        + [
            pltpu.VMEM((512, 128), F32),
            pltpu.VMEM((512, 128), F32),
            pltpu.VMEM((2, 256, 128), F32),
            pltpu.VMEM(total, F32),
            pltpu.SemaphoreType.DMA((7,)),
            pltpu.SemaphoreType.DMA((7,)),
            pltpu.SemaphoreType.DMA((7,)),
        ],
        compiler_params=pltpu.CompilerParams(
            collective_id=0, has_side_effects=True, vmem_limit_bytes=67043328 - 11300000
        ),
    )(
        activation.reshape(256, 8, 256),
        cotangent.reshape(256, 8, 256),
        spectral_weight.reshape(64, 64, 128),
        packed,
    )
    grad, wgrad = pl.pallas_call(
        expand,
        out_shape=(jax.ShapeDtypeStruct((256, 8, 256), BF16), jax.ShapeDtypeStruct(total, F32)),
        in_specs=[pl.BlockSpec(memory_space=pltpu.VMEM)] * 3,
        out_specs=[pl.BlockSpec(memory_space=pltpu.HBM)] * 2,
        scratch_shapes=[
            pltpu.VMEM((2, 512, 128), F32),
            pltpu.VMEM((2, 2, 1024, 128), F32),
            pltpu.VMEM((2, 128, 8, 256), BF16),
            pltpu.SemaphoreType.DMA((3,)),
        ],
        compiler_params=pltpu.CompilerParams(vmem_limit_bytes=20 << 20),
    )(got, ty, wgrad)
    return grad.reshape(4, 64, 8, 256), wgrad.reshape(2, 2, 32, 128)


def solution(mesh):
    placed = (P("dp", None, "slab", None), P("dp", None, "slab", None), P(None, "slab", None, None))
    return jax.shard_map(
        functools.partial(body, slabs=mesh.shape["slab"], groups=mesh.shape["dp"]),
        mesh=mesh,
        in_specs=placed,
        out_specs=(P("dp", None, "slab", None), P("dp", "slab", None, None)),
        check_vma=False,
    )
```

```python
import functools

import jax
import jax.numpy as jnp
import numpy as np
from jax import lax
from jax.experimental import pallas as pl
from jax.experimental.pallas import tpu as pltpu
from jax.sharding import PartitionSpec as P

MESH = pl.DeviceIdType.MESH
F32 = jnp.float32
BF16 = jnp.bfloat16


def retained(length, modes):
    index = np.arange(modes)
    return np.where(index < modes // 2, index, index + (length - modes))


def cos_sin(length, modes):
    phase = np.arange(length)[:, None] * retained(length, modes)[None, :] % length
    angle = phase * (2.0 * np.pi / length)
    factor = 1.0 / np.sqrt(length)
    return np.cos(angle) * factor, np.sin(angle) * factor


def tables(slabs):
    cos_y, sin_y = cos_sin(128, 32)
    table_y = np.concatenate(
        [np.concatenate([cos_y, -sin_y], 1), np.concatenate([sin_y, cos_y], 1)], 0
    )
    ty = table_y.reshape(256, 2, slabs, 32 // slabs).transpose(2, 3, 1, 0).reshape(64, 256)
    cos_x, sin_x = cos_sin(128, 32)
    table_x = np.stack(
        [np.stack([cos_x, -sin_x], 2), np.stack([sin_x, cos_x], 2)], 1
    )
    fx = table_x.reshape(slabs, 128 // slabs, 2, 32, 2).transpose(4, 3, 0, 2, 1).reshape(64, 256)
    packed = np.zeros((2048, 256), np.float32)
    packed[0:64], packed[64:128], packed[128:384, 0:64] = ty, fx, fx.T
    return jnp.asarray(ty, BF16), jnp.asarray(packed, BF16)


RING = (4, 3, 5, 2, 6, 1, 7, 0)


def dp_peers(me):
    part, along, core = lax.div(me, 16), lax.rem(lax.div(me, 2), 8), lax.rem(me, 2)
    parts = [lax.rem(part + n, 2) * 16 for n in range(2)]
    cores = [lax.rem(core + n, 2) for n in range(2)]
    peers = []
    for off in RING:
        row = lax.rem(along + off, 8) * 2
        peers += [row + parts[n] + cores[c] for n in (1, 0) for c in (1, 0)]
    return peers[:-1]


def nt(a, b):
    return lax.dot_general(a, b, (((1,), (1,)), ((), ())), preferred_element_type=F32)


def tn(a, b):
    return lax.dot_general(a, b, (((0,), (0,)), ((), ())), preferred_element_type=F32)


def kernel(
    slabs, groups,
    act_hbm, cot_hbm, w_hbm, tab_hbm,
    grad_ref, wgrad_ref,
    ty_ref, fx_ref, tx_ref, act_v, cot_v, w_v, wm, lines, folded,
    send_a, send_c, got_a, got_c, send_e, got_e,
    spectra, pair_a, pair_c, all_a, all_c, stacked, mixed, sums, wsend,
    load_sem, send_sem, recv_sem, ready, ready_d,
):
    me_s = lax.axis_index("slab")
    me_d = lax.axis_index("dp")

    loads = [
        pltpu.make_async_copy(src, dst, load_sem.at[n])
        for n, (src, dst) in enumerate(
            (
                (tab_hbm.at[pl.ds(0, 64)], ty_ref),
                (cot_hbm.at[pl.ds(0, 128)], cot_v.at[pl.ds(0, 128)]),
                (cot_hbm.at[pl.ds(128, 128)], cot_v.at[pl.ds(128, 128)]),
                (act_hbm, act_v), (w_hbm, w_v),
                (tab_hbm.at[pl.ds(64, 64)], fx_ref),
                (tab_hbm.at[pl.ds(128, 256), pl.ds(0, 128)], tx_ref),
            )
        )
    ]
    for load in loads:
        load.start()

    peers_d = dp_peers(me_d)
    barrier = pltpu.get_barrier_semaphore()
    part, mine = lax.div(me_s, 8), lax.rem(me_s, 8)
    levels = slabs // 2
    partner = lax.rem(part + 1, 2) * 8 + mine

    def to_slab(sem, peer):
        pl.semaphore_signal(sem, inc=1, device_id={"slab": peer}, device_id_type=MESH)

    def to_dp(sem, peer):
        pl.semaphore_signal(sem, inc=1, device_id={"dp": peer}, device_id_type=MESH)

    for level in range(1, levels):
        @pl.when(mine < level)
        def _():
            for n in range(2):
                to_slab(barrier, n * 8 + level)

    to_slab(barrier, partner)

    for peer in range(1, groups):
        @pl.when(me_d < peer)
        def _():
            to_dp(barrier, peer)

    pl.semaphore_wait(barrier, 2 * mine + 1 + me_d)
    for level in range(levels - 1):
        @pl.when(level < mine)
        def _():
            for n in range(2):
                to_slab(ready.at[mine], n * 8 + level)

    for peer in range(groups - 1):
        @pl.when(peer < me_d)
        def _():
            to_dp(ready_d, peer)


    def send_slab(peer, src, dst, n):
        pltpu.make_async_remote_copy(
            src_ref=src.at[:, peer], dst_ref=dst.at[:, me_s],
            send_sem=send_sem.at[n], recv_sem=recv_sem.at[n],
            device_id={"slab": peer}, device_id_type=MESH,
        ).start()

    def send_earlier(src, dst, n):
        send_slab(partner, src, dst, n)
        for level in range(levels - 1):
            @pl.when(level < mine)
            def _():
                for half in range(2):
                    send_slab(half * 8 + level, src, dst, n)

    def exchange(axis, me, peers, src, dst, n, rank=0):
        lead = (slice(None),) * rank
        for peer in peers:
            pltpu.make_async_remote_copy(
                src_ref=src.at[(*lead, peer)], dst_ref=dst.at[(*lead, me)],
                send_sem=send_sem.at[n], recv_sem=recv_sem.at[n],
                device_id={axis: peer}, device_id_type=MESH,
            ).start()

    def wait_all(ref, count, sem):
        part = ref.at[pl.ds(0, count - 1)] if ref.shape[0] == count else ref.at[:, pl.ds(0, count - 1)]
        pltpu.make_async_copy(part, part, sem).wait()


    def over_slab(src, dst, n):
        for off in RING[:-1]:
            for half in range(2):
                send_slab(half * 8 + lax.rem(mine + off, 8), src, dst, n)
        send_slab(partner, src, dst, n)

    over_dp = functools.partial(exchange, "dp", me_d, peers_d)

    def along_y(field, send, h):
        for c in range(4):
            part = field[h * 128 + c * 32 : h * 128 + (c + 1) * 32].astype(F32).reshape(256, 256)
            for half in range(2):
                lines[half, c * 256 : (c + 1) * 256, :] = part[:, half * 128 : half * 128 + 128]
        for r in range(8):
            rows = jnp.concatenate(
                [lines[half, pl.ds(r, 128, stride=8), :] for half in range(2)], axis=1
            ).astype(BF16)
            folded[pl.ds(r, 64, stride=8), :] = nt(ty_ref[...], rows)
        send[h] = folded[...].astype(BF16).reshape(slabs, 2, 16, 128)

    loads[0].wait()
    loads[1].wait()
    along_y(cot_v, send_c, 0)
    loads[2].wait()
    along_y(cot_v, send_c, 1)
    send_earlier(send_c, got_c, 0)
    for h in range(2):
        got_c[h, me_s] = send_c[h, me_s]
    loads[3].wait()
    along_y(act_v, send_a, 0)
    along_y(act_v, send_a, 1)
    send_earlier(send_a, got_a, 2)
    for h in range(2):
        got_a[h, me_s] = send_a[h, me_s]
    for level in range(1, levels):
        @pl.when(mine < level)
        def _():
            pl.semaphore_wait(ready.at[level], 2)
            for half in range(2):
                send_slab(half * 8 + level, send_c, got_c, 0)
            for half in range(2):
                send_slab(half * 8 + level, send_a, got_a, 2)

    loads[4].wait()
    for c in range(8):
        part = w_v[c * 8 : (c + 1) * 8].astype(F32).reshape(512, 128)
        lines[c // 4, c % 4 * 512 : (c % 4 + 1) * 512, :] = part

    @pl.loop(0, 64)
    def _(m):
        for half in range(2):
            wm[m, half * 32 : half * 32 + 32, :] = lines[
                half, pl.ds(m, 32, stride=64), :
            ].astype(BF16)

    lane = lax.broadcasted_iota(jnp.int32, (32, 128), 1)
    low = lane < 64

    def spec_of(got):
        return [
            [
                jnp.dot(fx_ref[...], got[h, :, t].reshape(256, 128), preferred_element_type=F32)
                .astype(BF16)
                .astype(F32)
                for h in range(2)
            ]
            for t in range(2)
        ]

    def to_pair(specs, pair):
        for t in range(2):
            for q in range(2):
                for h in range(2):
                    spectra[pl.ds(t * 128 + q * 2 + h, 32, stride=4), :] = specs[t][h][
                        q * 32 : q * 32 + 32
                    ]
        pair[...] = spectra[...].astype(BF16).reshape(groups, 256 // groups, 128)

    wait_all(got_c, slabs, recv_sem.at[0])
    loads[5].wait()
    loads[6].wait()
    specs = spec_of(got_c)

    for t in range(2):
        for h in range(2):
            re, im = specs[t][h][0:32], specs[t][h][32:64]
            re_r = pltpu.roll(re, 64, 1)
            im_r = pltpu.roll(im, 64, 1)
            rows = (
                jnp.where(low, re, im_r),
                jnp.where(low, im, -re_r),
                jnp.where(low, re_r, im),
                jnp.where(low, im_r, -re),
            )
            for n, row in enumerate(rows):
                stacked[pl.ds(t * 256 + h * 4 + n, 32, stride=8), :] = row

    for n in range(16):
        both = nt(
            stacked[n * 32 : n * 32 + 32, :].astype(BF16),
            wm[n * 4 : n * 4 + 4].reshape(256, 128),
        )
        for m in range(4):
            block = both[m * 8 : m * 8 + 8, m // 2 * 128 : m // 2 * 128 + 128]
            mixed[n * 32 + m * 8 : n * 32 + m * 8 + 8, :] = (
                pltpu.roll(block, 64, 1) if m % 2 else block
            )

    for t in range(2):
        rows = []
        for q in range(2):
            tiles = []
            for h in range(2):
                first = mixed[pl.ds(t * 256 + h * 4 + q, 32, stride=8), :]
                second = mixed[pl.ds(t * 256 + h * 4 + 2 + q, 32, stride=8), :]
                tiles.append(jnp.where(low, first, pltpu.roll(second, 64, 1)))
            rows.append(jnp.concatenate(tiles, axis=1))
        grads = jnp.concatenate(rows, axis=0).astype(BF16)
        spread = jnp.dot(tx_ref[:, 0:64], grads, preferred_element_type=F32)
        for h in range(2):
            send_e[h, :, t] = (
                spread[:, h * 128 : h * 128 + 128].astype(BF16).reshape(slabs, 16, 128)
            )
    for h in range(2):
        got_e[h, me_s] = send_e[h, me_s]

    to_pair(specs, pair_c)
    all_c[me_d] = pair_c[me_d]
    @pl.when(me_d < groups - 1)
    def _():
        pl.semaphore_wait(ready_d, groups - 1 - me_d)

    over_dp(pair_c, all_c, 4)

    wait_all(got_a, slabs, recv_sem.at[2])
    to_pair(spec_of(got_a), pair_a)
    all_a[me_d] = pair_a[me_d]
    over_dp(pair_a, all_a, 5)
    over_slab(send_e, got_e, 3)

    wait_all(all_c, groups, recv_sem.at[4])
    wait_all(all_a, groups, recv_sem.at[5])
    sums[0] = all_a[...].astype(F32).reshape(256, 128)
    sums[1] = all_c[...].astype(F32).reshape(256, 128)
    wide = lax.broadcasted_iota(jnp.int32, (64, 128), 1) < 64
    for m in range(2):
        def part(which, q):
            return jnp.concatenate(
                [sums[which, pl.ds(m * 4 + q * 2 + h, groups, stride=8), :] for h in range(2)],
                axis=0,
            )

        ins = jnp.concatenate([part(0, 0), part(0, 1)], axis=0).astype(BF16)
        out_re, out_im = part(1, 0), part(1, 1)
        outs = jnp.concatenate([out_re, out_im], axis=0)
        swapped = jnp.concatenate([out_im, -out_re], axis=0)
        prod = tn(ins, jnp.concatenate([outs, swapped], axis=1).astype(BF16))
        top, bottom = prod[0:64], prod[64:128]
        total = jnp.where(
            wide,
            top[:, 0:128] + pltpu.roll(bottom[:, 0:128], 64, 1),
            pltpu.roll(top[:, 128:256], 64, 1) + bottom[:, 128:256],
        )
        mixed[m * 64 : m * 64 + 64, :] = total
    for m in range(2):
        for i in range(2):
            wsend[i, :, m, :] = mixed[pl.ds(m * 64 + i, groups, stride=2), :]
    for i in range(2):
        wgrad_ref[i, me_d] = wsend[i, me_d]
    over_dp(wsend, wgrad_ref, 6, rank=1)

    wait_all(got_e, slabs, recv_sem.at[3])
    for h in range(2):
        folded[...] = got_e[h].astype(F32).reshape(512, 128)
        for r in range(8):
            values = tn(folded[pl.ds(r, 64, stride=8), :].astype(BF16), ty_ref[...])
            for half in range(2):
                lines[half, pl.ds(r, 128, stride=8), :] = values[
                    :, half * 128 : half * 128 + 128
                ]
        for c in range(4):
            grad_ref[h * 128 + c * 32 : h * 128 + (c + 1) * 32] = (
                jnp.concatenate(
                    [lines[half, c * 256 : (c + 1) * 256, :] for half in range(2)], axis=1
                )
                .astype(BF16)
                .reshape(32, 8, 256)
            )
    wait_all(wgrad_ref, groups, recv_sem.at[6])
    for n, ref in ((0, send_c), (2, send_a), (3, send_e)):
        wait_all(ref, slabs, send_sem.at[n])
    for n, ref in enumerate((pair_c, pair_a, wsend)):
        wait_all(ref, groups, send_sem.at[4 + n])


def passed(grad_ref, wgrad_ref, grad_hbm, wgrad_hbm, sems):
    copies = [
        pltpu.make_async_copy(grad_ref, grad_hbm, sems.at[0]),
        pltpu.make_async_copy(wgrad_ref, wgrad_hbm, sems.at[1]),
    ]
    for copy in copies:
        copy.start()
    for copy in copies:
        copy.wait()


def body(activation, cotangent, spectral_weight, slabs, groups):
    ty, packed = tables(slabs)
    block = (2, slabs, 2, 16, 128)
    pair = (groups, 256 // groups, 128)
    total = (2, groups, 2, 128)
    got, wgrad = pl.pallas_call(
        functools.partial(kernel, slabs, groups),
        out_shape=(
            jax.ShapeDtypeStruct((256, 8, 256), BF16),
            jax.ShapeDtypeStruct(total, F32),
        ),
        in_specs=[pl.BlockSpec(memory_space=pltpu.HBM)] * 4,
        out_specs=[pl.BlockSpec(memory_space=pltpu.VMEM)] * 2,
        scratch_shapes=[
            pltpu.VMEM((64, 256), BF16),
            pltpu.VMEM((64, 256), BF16),
            pltpu.VMEM((256, 128), BF16),
            pltpu.VMEM((256, 8, 256), BF16),
            pltpu.VMEM((256, 8, 256), BF16),
            pltpu.VMEM((64, 64, 128), BF16),
            pltpu.VMEM((64, 64, 128), BF16),
            pltpu.VMEM((2, 2048, 128), F32),
            pltpu.VMEM((512, 128), F32),
        ]
        + [pltpu.VMEM(block, BF16)] * 6
        + [pltpu.VMEM((256, 128), F32)]
        + [pltpu.VMEM(pair, BF16)] * 4
        + [
            pltpu.VMEM((512, 128), F32),
            pltpu.VMEM((512, 128), F32),
            pltpu.VMEM((2, 256, 128), F32),
            pltpu.VMEM(total, F32),
            pltpu.SemaphoreType.DMA((7,)),
            pltpu.SemaphoreType.DMA((7,)),
            pltpu.SemaphoreType.DMA((7,)),
            pltpu.SemaphoreType.REGULAR((slabs // 2,)),
            pltpu.SemaphoreType.REGULAR,
        ],
        compiler_params=pltpu.CompilerParams(
            collective_id=0, has_side_effects=True, vmem_limit_bytes=67043328 - 12200000
        ),
    )(
        activation.reshape(256, 8, 256),
        cotangent.reshape(256, 8, 256),
        spectral_weight.reshape(64, 64, 128),
        packed,
    )
    grad, wgrad = pl.pallas_call(
        passed,
        out_shape=(jax.ShapeDtypeStruct((256, 8, 256), BF16), jax.ShapeDtypeStruct(total, F32)),
        in_specs=[pl.BlockSpec(memory_space=pltpu.VMEM)] * 2,
        out_specs=[pl.BlockSpec(memory_space=pltpu.HBM)] * 2,
        scratch_shapes=[pltpu.SemaphoreType.DMA((2,))],
        compiler_params=pltpu.CompilerParams(vmem_limit_bytes=20 << 20),
    )(got, wgrad)
    return grad.reshape(4, 64, 8, 256), wgrad.reshape(2, 2, 32, 128)


def solution(mesh):
    placed = (P("dp", None, "slab", None), P("dp", None, "slab", None), P(None, "slab", None, None))
    return jax.shard_map(
        functools.partial(body, slabs=mesh.shape["slab"], groups=mesh.shape["dp"]),
        mesh=mesh,
        in_specs=placed,
        out_specs=(P("dp", None, "slab", None), P("dp", "slab", None, None)),
        check_vma=False,
    )
```

```python
import functools

import jax
import jax.numpy as jnp
import numpy as np
from jax import lax
from jax.experimental import pallas as pl
from jax.experimental.pallas import tpu as pltpu
from jax.sharding import PartitionSpec as P

MESH = pl.DeviceIdType.MESH
F32 = jnp.float32
BF16 = jnp.bfloat16


def retained(length, modes):
    index = np.arange(modes)
    return np.where(index < modes // 2, index, index + (length - modes))


def cos_sin(length, modes):
    phase = np.arange(length)[:, None] * retained(length, modes)[None, :] % length
    angle = phase * (2.0 * np.pi / length)
    factor = 1.0 / np.sqrt(length)
    return np.cos(angle) * factor, np.sin(angle) * factor


def tables(slabs):
    cos_y, sin_y = cos_sin(128, 32)
    table_y = np.concatenate(
        [np.concatenate([cos_y, -sin_y], 1), np.concatenate([sin_y, cos_y], 1)], 0
    )
    ty = table_y.reshape(256, 2, slabs, 32 // slabs).transpose(2, 3, 1, 0).reshape(64, 256)
    cos_x, sin_x = cos_sin(128, 32)
    table_x = np.stack(
        [np.stack([cos_x, -sin_x], 2), np.stack([sin_x, cos_x], 2)], 1
    )
    fx = table_x.reshape(slabs, 128 // slabs, 2, 32, 2).transpose(4, 3, 0, 2, 1).reshape(64, 256)
    packed = np.zeros((2048, 256), np.float32)
    packed[0:64], packed[64:128], packed[128:384, 0:64] = ty, fx, fx.T
    return jnp.asarray(ty, BF16), jnp.asarray(packed, BF16)


RING = (4, 3, 5, 2, 6, 1, 7, 0)


def dp_peers(me):
    part, along, core = lax.div(me, 16), lax.rem(lax.div(me, 2), 8), lax.rem(me, 2)
    parts = [lax.rem(part + n, 2) * 16 for n in range(2)]
    cores = [lax.rem(core + n, 2) for n in range(2)]
    peers = []
    for off in RING:
        row = lax.rem(along + off, 8) * 2
        peers += [row + parts[n] + cores[c] for n in (1, 0) for c in (1, 0)]
    return peers[:-1]


def nt(a, b):
    return lax.dot_general(a, b, (((1,), (1,)), ((), ())), preferred_element_type=F32)


def tn(a, b):
    return lax.dot_general(a, b, (((0,), (0,)), ((), ())), preferred_element_type=F32)


def kernel(
    slabs, groups,
    act_hbm, cot_hbm, w_hbm, tab_hbm,
    grad_ref, wgrad_ref,
    ty_ref, fx_ref, tx_ref, act_v, cot_v, w_v, wm, lines, folded,
    send_a, send_c, got_a, got_c, send_e, got_e,
    spectra, pair_a, pair_c, all_a, all_c, stacked, mixed, sums, wsend,
    load_sem, send_sem, recv_sem, ready, near, four, passed_on,
):
    me_s = lax.axis_index("slab")
    me_d = lax.axis_index("dp")

    loads = [
        pltpu.make_async_copy(src, dst, load_sem.at[n])
        for n, (src, dst) in enumerate(
            (
                (tab_hbm.at[pl.ds(0, 64)], ty_ref),
                (cot_hbm.at[pl.ds(0, 128)], cot_v.at[pl.ds(0, 128)]),
                (cot_hbm.at[pl.ds(128, 128)], cot_v.at[pl.ds(128, 128)]),
                (act_hbm, act_v), (w_hbm, w_v),
                (tab_hbm.at[pl.ds(64, 64)], fx_ref),
                (tab_hbm.at[pl.ds(128, 256), pl.ds(0, 128)], tx_ref),
            )
        )
    ]
    for load in loads:
        load.start()

    peers_d = dp_peers(me_d)
    rows_y = groups // 4
    barrier = pltpu.get_barrier_semaphore()
    part, mine = lax.div(me_s, 8), lax.rem(me_s, 8)
    levels = slabs // 2
    partner = lax.rem(part + 1, 2) * 8 + mine

    def to_slab(sem, peer):
        pl.semaphore_signal(sem, inc=1, device_id={"slab": peer}, device_id_type=MESH)

    def to_dp(sem, peer):
        pl.semaphore_signal(sem, inc=1, device_id={"dp": peer}, device_id_type=MESH)

    for level in range(1, levels):
        @pl.when(mine < level)
        def _():
            for n in range(2):
                to_slab(barrier, n * 8 + level)

    to_slab(barrier, partner)

    core, row, side = lax.rem(me_d, 2), lax.rem(lax.div(me_d, 2), rows_y), lax.div(me_d, 2 * rows_y)
    last = rows_y - 1
    for earlier, step in ((core == 0, 1), (side == 0, 2 * rows_y), (row < last, 2)):
        @pl.when(earlier)
        def _():
            to_dp(barrier, me_d + step)

    pl.semaphore_wait(barrier, 2 * mine + 1 + core + side + lax.div(row + last, rows_y))
    for level in range(levels - 1):
        @pl.when(level < mine)
        def _():
            for n in range(2):
                to_slab(ready.at[mine], n * 8 + level)

    for later, step in ((core == 1, 1), (side == 1, 2 * rows_y), (row > 0, 2)):
        @pl.when(later)
        def _():
            to_dp(near, me_d - step)


    def meet_four():
        count = 2 - core - side + lax.div(2 * last - row - 1, last)

        @pl.when(count > 0)
        def _():
            pl.semaphore_wait(near, count)

        to_dp(four, side * 2 * rows_y + row * 2 + 1 - core)
        to_dp(four, (1 - side) * 2 * rows_y + row * 2 + core)

    def scan(upward):
        first, final = (row > 0, row < last) if upward else (row < last, row > 0)

        @pl.when(first)
        def _():
            pl.semaphore_wait(passed_on.at[int(upward)], 1)

        @pl.when(final)
        def _():
            to_dp(passed_on.at[int(upward)], me_d + 2 if upward else me_d - 2)

    def meet_half(which):
        for low_half in (True, False):
            @pl.when((row < rows_y // 2) if low_half else (row >= rows_y // 2))
            def _():
                scan(low_half == (which == 0))

    def send_slab(peer, src, dst, n):
        pltpu.make_async_remote_copy(
            src_ref=src.at[:, peer], dst_ref=dst.at[:, me_s],
            send_sem=send_sem.at[n], recv_sem=recv_sem.at[n],
            device_id={"slab": peer}, device_id_type=MESH,
        ).start()

    def send_earlier(src, dst, n):
        send_slab(partner, src, dst, n)
        for level in range(levels - 1):
            @pl.when(level < mine)
            def _():
                for half in range(2):
                    send_slab(half * 8 + level, src, dst, n)

    def exchange(axis, me, peers, src, dst, n, rank=0):
        lead = (slice(None),) * rank
        for peer in peers:
            pltpu.make_async_remote_copy(
                src_ref=src.at[(*lead, peer)], dst_ref=dst.at[(*lead, me)],
                send_sem=send_sem.at[n], recv_sem=recv_sem.at[n],
                device_id={axis: peer}, device_id_type=MESH,
            ).start()

    def wait_all(ref, count, sem):
        part = ref.at[pl.ds(0, count - 1)] if ref.shape[0] == count else ref.at[:, pl.ds(0, count - 1)]
        pltpu.make_async_copy(part, part, sem).wait()


    def over_slab(src, dst, n):
        for off in RING[:-1]:
            for half in range(2):
                send_slab(half * 8 + lax.rem(mine + off, 8), src, dst, n)
        send_slab(partner, src, dst, n)

    over_dp = functools.partial(exchange, "dp", me_d, peers_d)

    def along_y(field, send, h):
        for c in range(4):
            part = field[h * 128 + c * 32 : h * 128 + (c + 1) * 32].astype(F32).reshape(256, 256)
            for half in range(2):
                lines[half, c * 256 : (c + 1) * 256, :] = part[:, half * 128 : half * 128 + 128]
        for r in range(8):
            rows = jnp.concatenate(
                [lines[half, pl.ds(r, 128, stride=8), :] for half in range(2)], axis=1
            ).astype(BF16)
            folded[pl.ds(r, 64, stride=8), :] = nt(ty_ref[...], rows)
        send[h] = folded[...].astype(BF16).reshape(slabs, 2, 16, 128)

    loads[0].wait()
    loads[1].wait()
    along_y(cot_v, send_c, 0)
    loads[2].wait()
    along_y(cot_v, send_c, 1)
    send_earlier(send_c, got_c, 0)
    for h in range(2):
        got_c[h, me_s] = send_c[h, me_s]
    loads[3].wait()
    along_y(act_v, send_a, 0)
    along_y(act_v, send_a, 1)
    send_earlier(send_a, got_a, 2)
    for h in range(2):
        got_a[h, me_s] = send_a[h, me_s]
    meet_four()
    for level in range(1, levels):
        @pl.when(mine < level)
        def _():
            pl.semaphore_wait(ready.at[level], 2)
            for half in range(2):
                send_slab(half * 8 + level, send_c, got_c, 0)
            for half in range(2):
                send_slab(half * 8 + level, send_a, got_a, 2)

    pl.semaphore_wait(four, 2)
    meet_half(0)
    loads[4].wait()
    for c in range(8):
        part = w_v[c * 8 : (c + 1) * 8].astype(F32).reshape(512, 128)
        lines[c // 4, c % 4 * 512 : (c % 4 + 1) * 512, :] = part

    @pl.loop(0, 64)
    def _(m):
        for half in range(2):
            wm[m, half * 32 : half * 32 + 32, :] = lines[
                half, pl.ds(m, 32, stride=64), :
            ].astype(BF16)

    lane = lax.broadcasted_iota(jnp.int32, (32, 128), 1)
    low = lane < 64

    def spec_of(got):
        return [
            [
                jnp.dot(fx_ref[...], got[h, :, t].reshape(256, 128), preferred_element_type=F32)
                .astype(BF16)
                .astype(F32)
                for h in range(2)
            ]
            for t in range(2)
        ]

    def to_pair(specs, pair):
        for t in range(2):
            for q in range(2):
                for h in range(2):
                    spectra[pl.ds(t * 128 + q * 2 + h, 32, stride=4), :] = specs[t][h][
                        q * 32 : q * 32 + 32
                    ]
        pair[...] = spectra[...].astype(BF16).reshape(groups, 256 // groups, 128)

    meet_half(1)
    wait_all(got_c, slabs, recv_sem.at[0])
    loads[5].wait()
    loads[6].wait()
    specs = spec_of(got_c)

    for t in range(2):
        for h in range(2):
            re, im = specs[t][h][0:32], specs[t][h][32:64]
            re_r = pltpu.roll(re, 64, 1)
            im_r = pltpu.roll(im, 64, 1)
            rows = (
                jnp.where(low, re, im_r),
                jnp.where(low, im, -re_r),
                jnp.where(low, re_r, im),
                jnp.where(low, im_r, -re),
            )
            for n, row in enumerate(rows):
                stacked[pl.ds(t * 256 + h * 4 + n, 32, stride=8), :] = row

    for n in range(16):
        both = nt(
            stacked[n * 32 : n * 32 + 32, :].astype(BF16),
            wm[n * 4 : n * 4 + 4].reshape(256, 128),
        )
        for m in range(4):
            block = both[m * 8 : m * 8 + 8, m // 2 * 128 : m // 2 * 128 + 128]
            mixed[n * 32 + m * 8 : n * 32 + m * 8 + 8, :] = (
                pltpu.roll(block, 64, 1) if m % 2 else block
            )

    for t in range(2):
        rows = []
        for q in range(2):
            tiles = []
            for h in range(2):
                first = mixed[pl.ds(t * 256 + h * 4 + q, 32, stride=8), :]
                second = mixed[pl.ds(t * 256 + h * 4 + 2 + q, 32, stride=8), :]
                tiles.append(jnp.where(low, first, pltpu.roll(second, 64, 1)))
            rows.append(jnp.concatenate(tiles, axis=1))
        grads = jnp.concatenate(rows, axis=0).astype(BF16)
        spread = jnp.dot(tx_ref[:, 0:64], grads, preferred_element_type=F32)
        for h in range(2):
            send_e[h, :, t] = (
                spread[:, h * 128 : h * 128 + 128].astype(BF16).reshape(slabs, 16, 128)
            )
    for h in range(2):
        got_e[h, me_s] = send_e[h, me_s]

    to_pair(specs, pair_c)
    all_c[me_d] = pair_c[me_d]
    over_dp(pair_c, all_c, 4)

    wait_all(got_a, slabs, recv_sem.at[2])
    to_pair(spec_of(got_a), pair_a)
    all_a[me_d] = pair_a[me_d]
    over_dp(pair_a, all_a, 5)
    over_slab(send_e, got_e, 3)

    wait_all(all_c, groups, recv_sem.at[4])
    wait_all(all_a, groups, recv_sem.at[5])
    sums[0] = all_a[...].astype(F32).reshape(256, 128)
    sums[1] = all_c[...].astype(F32).reshape(256, 128)
    wide = lax.broadcasted_iota(jnp.int32, (64, 128), 1) < 64
    for m in range(2):
        def part(which, q):
            return jnp.concatenate(
                [sums[which, pl.ds(m * 4 + q * 2 + h, groups, stride=8), :] for h in range(2)],
                axis=0,
            )

        ins = jnp.concatenate([part(0, 0), part(0, 1)], axis=0).astype(BF16)
        out_re, out_im = part(1, 0), part(1, 1)
        outs = jnp.concatenate([out_re, out_im], axis=0)
        swapped = jnp.concatenate([out_im, -out_re], axis=0)
        prod = tn(ins, jnp.concatenate([outs, swapped], axis=1).astype(BF16))
        top, bottom = prod[0:64], prod[64:128]
        total = jnp.where(
            wide,
            top[:, 0:128] + pltpu.roll(bottom[:, 0:128], 64, 1),
            pltpu.roll(top[:, 128:256], 64, 1) + bottom[:, 128:256],
        )
        mixed[m * 64 : m * 64 + 64, :] = total
    for m in range(2):
        for i in range(2):
            wsend[i, :, m, :] = mixed[pl.ds(m * 64 + i, groups, stride=2), :]
    for i in range(2):
        wgrad_ref[i, me_d] = wsend[i, me_d]
    over_dp(wsend, wgrad_ref, 6, rank=1)

    wait_all(got_e, slabs, recv_sem.at[3])
    for h in range(2):
        folded[...] = got_e[h].astype(F32).reshape(512, 128)
        for r in range(8):
            values = tn(folded[pl.ds(r, 64, stride=8), :].astype(BF16), ty_ref[...])
            for half in range(2):
                lines[half, pl.ds(r, 128, stride=8), :] = values[
                    :, half * 128 : half * 128 + 128
                ]
        for c in range(4):
            grad_ref[h * 128 + c * 32 : h * 128 + (c + 1) * 32] = (
                jnp.concatenate(
                    [lines[half, c * 256 : (c + 1) * 256, :] for half in range(2)], axis=1
                )
                .astype(BF16)
                .reshape(32, 8, 256)
            )
    wait_all(wgrad_ref, groups, recv_sem.at[6])
    for n, ref in ((0, send_c), (2, send_a), (3, send_e)):
        wait_all(ref, slabs, send_sem.at[n])
    for n, ref in enumerate((pair_c, pair_a, wsend)):
        wait_all(ref, groups, send_sem.at[4 + n])


def write_out(grad_ref, wgrad_ref, grad_hbm, wgrad_hbm, sems):
    copies = [
        pltpu.make_async_copy(grad_ref, grad_hbm, sems.at[0]),
        pltpu.make_async_copy(wgrad_ref, wgrad_hbm, sems.at[1]),
    ]
    for copy in copies:
        copy.start()
    for copy in copies:
        copy.wait()


def body(activation, cotangent, spectral_weight, slabs, groups):
    ty, packed = tables(slabs)
    block = (2, slabs, 2, 16, 128)
    pair = (groups, 256 // groups, 128)
    total = (2, groups, 2, 128)
    got, wgrad = pl.pallas_call(
        functools.partial(kernel, slabs, groups),
        out_shape=(
            jax.ShapeDtypeStruct((256, 8, 256), BF16),
            jax.ShapeDtypeStruct(total, F32),
        ),
        in_specs=[pl.BlockSpec(memory_space=pltpu.HBM)] * 4,
        out_specs=[pl.BlockSpec(memory_space=pltpu.VMEM)] * 2,
        scratch_shapes=[
            pltpu.VMEM((64, 256), BF16),
            pltpu.VMEM((64, 256), BF16),
            pltpu.VMEM((256, 128), BF16),
            pltpu.VMEM((256, 8, 256), BF16),
            pltpu.VMEM((256, 8, 256), BF16),
            pltpu.VMEM((64, 64, 128), BF16),
            pltpu.VMEM((64, 64, 128), BF16),
            pltpu.VMEM((2, 2048, 128), F32),
            pltpu.VMEM((512, 128), F32),
        ]
        + [pltpu.VMEM(block, BF16)] * 6
        + [pltpu.VMEM((256, 128), F32)]
        + [pltpu.VMEM(pair, BF16)] * 4
        + [
            pltpu.VMEM((512, 128), F32),
            pltpu.VMEM((512, 128), F32),
            pltpu.VMEM((2, 256, 128), F32),
            pltpu.VMEM(total, F32),
            pltpu.SemaphoreType.DMA((7,)),
            pltpu.SemaphoreType.DMA((7,)),
            pltpu.SemaphoreType.DMA((7,)),
            pltpu.SemaphoreType.REGULAR((slabs // 2,)),
            pltpu.SemaphoreType.REGULAR,
            pltpu.SemaphoreType.REGULAR,
            pltpu.SemaphoreType.REGULAR((2,)),
        ],
        compiler_params=pltpu.CompilerParams(
            collective_id=0, has_side_effects=True, vmem_limit_bytes=67043328 - 12200000
        ),
    )(
        activation.reshape(256, 8, 256),
        cotangent.reshape(256, 8, 256),
        spectral_weight.reshape(64, 64, 128),
        packed,
    )
    grad, wgrad = pl.pallas_call(
        write_out,
        out_shape=(jax.ShapeDtypeStruct((256, 8, 256), BF16), jax.ShapeDtypeStruct(total, F32)),
        in_specs=[pl.BlockSpec(memory_space=pltpu.VMEM)] * 2,
        out_specs=[pl.BlockSpec(memory_space=pltpu.HBM)] * 2,
        scratch_shapes=[pltpu.SemaphoreType.DMA((2,))],
        compiler_params=pltpu.CompilerParams(vmem_limit_bytes=20 << 20),
    )(got, wgrad)
    return grad.reshape(4, 64, 8, 256), wgrad.reshape(2, 2, 32, 128)


def solution(mesh):
    placed = (P("dp", None, "slab", None), P("dp", None, "slab", None), P(None, "slab", None, None))
    return jax.shard_map(
        functools.partial(body, slabs=mesh.shape["slab"], groups=mesh.shape["dp"]),
        mesh=mesh,
        in_specs=placed,
        out_specs=(P("dp", None, "slab", None), P("dp", "slab", None, None)),
        check_vma=False,
    )
```

```python
import functools

import jax
import jax.numpy as jnp
import numpy as np
from jax import lax
from jax.experimental import pallas as pl
from jax.experimental.pallas import tpu as pltpu
from jax.sharding import PartitionSpec as P

MESH = pl.DeviceIdType.MESH
F32 = jnp.float32
BF16 = jnp.bfloat16


def retained(length, modes):
    index = np.arange(modes)
    return np.where(index < modes // 2, index, index + (length - modes))


def cos_sin(length, modes):
    phase = np.arange(length)[:, None] * retained(length, modes)[None, :] % length
    angle = phase * (2.0 * np.pi / length)
    factor = 1.0 / np.sqrt(length)
    return np.cos(angle) * factor, np.sin(angle) * factor


def tables(slabs):
    cos_y, sin_y = cos_sin(128, 32)
    table_y = np.concatenate(
        [np.concatenate([cos_y, -sin_y], 1), np.concatenate([sin_y, cos_y], 1)], 0
    )
    ty = table_y.reshape(256, 2, slabs, 32 // slabs).transpose(2, 3, 1, 0).reshape(64, 256)
    cos_x, sin_x = cos_sin(128, 32)
    table_x = np.stack(
        [np.stack([cos_x, -sin_x], 2), np.stack([sin_x, cos_x], 2)], 1
    )
    fx = table_x.reshape(slabs, 128 // slabs, 2, 32, 2).transpose(4, 3, 0, 2, 1).reshape(64, 256)
    packed = np.zeros((2048, 256), np.float32)
    packed[0:64], packed[64:128], packed[128:384, 0:64] = ty, fx, fx.T
    return jnp.asarray(ty, BF16), jnp.asarray(packed, BF16)


RING = (4, 3, 5, 2, 6, 1, 7, 0)


def dp_peers(me):
    part, along, core = lax.div(me, 16), lax.rem(lax.div(me, 2), 8), lax.rem(me, 2)
    parts = [lax.rem(part + n, 2) * 16 for n in range(2)]
    cores = [lax.rem(core + n, 2) for n in range(2)]
    peers = []
    for off in RING:
        row = lax.rem(along + off, 8) * 2
        peers += [row + parts[n] + cores[c] for n in (1, 0) for c in (1, 0)]
    return peers[:-1]


def nt(a, b):
    return lax.dot_general(a, b, (((1,), (1,)), ((), ())), preferred_element_type=F32)


def tn(a, b):
    return lax.dot_general(a, b, (((0,), (0,)), ((), ())), preferred_element_type=F32)


def kernel(
    slabs, groups,
    act_hbm, cot_hbm, w_hbm, tab_hbm,
    grad_ref, wgrad_ref,
    ty_ref, fx_ref, tx_ref, act_v, cot_v, w_v, wm, lines, folded,
    send_a, send_c, got_a, got_c, send_e, got_e,
    spectra, pair_a, pair_c, all_a, all_c, stacked, mixed, sums, wsend,
    load_sem, send_sem, recv_sem, ready, near, four, passed_on,
):
    me_s = lax.axis_index("slab")
    me_d = lax.axis_index("dp")

    loads = [
        pltpu.make_async_copy(src, dst, load_sem.at[n])
        for n, (src, dst) in enumerate(
            (
                (tab_hbm.at[pl.ds(0, 64)], ty_ref),
                (cot_hbm.at[pl.ds(0, 128)], cot_v.at[pl.ds(0, 128)]),
                (cot_hbm.at[pl.ds(128, 128)], cot_v.at[pl.ds(128, 128)]),
                (act_hbm, act_v), (w_hbm, w_v),
                (tab_hbm.at[pl.ds(64, 64)], fx_ref),
                (tab_hbm.at[pl.ds(128, 256), pl.ds(0, 128)], tx_ref),
            )
        )
    ]
    for load in loads:
        load.start()

    peers_d = dp_peers(me_d)
    rows_y = groups // 4
    barrier = pltpu.get_barrier_semaphore()
    part, mine = lax.div(me_s, 8), lax.rem(me_s, 8)
    levels = slabs // 2
    partner = lax.rem(part + 1, 2) * 8 + mine

    def to_slab(sem, peer):
        pl.semaphore_signal(sem, inc=1, device_id={"slab": peer}, device_id_type=MESH)

    def to_dp(sem, peer):
        pl.semaphore_signal(sem, inc=1, device_id={"dp": peer}, device_id_type=MESH)

    for level in range(1, levels):
        @pl.when(mine < level)
        def _():
            for n in range(2):
                to_slab(barrier, n * 8 + level)

    to_slab(barrier, partner)

    core, row, side = lax.rem(me_d, 2), lax.rem(lax.div(me_d, 2), rows_y), lax.div(me_d, 2 * rows_y)
    last = rows_y - 1
    for earlier, step in ((core == 0, 1), (side == 0, 2 * rows_y), (row < last, 2)):
        @pl.when(earlier)
        def _():
            to_dp(barrier, me_d + step)

    pl.semaphore_wait(barrier, 2 * mine + 1 + core + side + lax.div(row + last, rows_y))
    for level in range(levels - 1):
        @pl.when(level < mine)
        def _():
            for n in range(2):
                to_slab(ready.at[mine], n * 8 + level)

    for later, step in ((core == 1, 1), (side == 1, 2 * rows_y), (row > 0, 2)):
        @pl.when(later)
        def _():
            to_dp(near, me_d - step)


    def meet_four():
        count = 2 - core - side + lax.div(2 * last - row - 1, last)

        @pl.when(count > 0)
        def _():
            pl.semaphore_wait(near, count)

        to_dp(four, side * 2 * rows_y + row * 2 + 1 - core)
        to_dp(four, (1 - side) * 2 * rows_y + row * 2 + core)

    def scan(upward):
        first, final = (row > 0, row < last) if upward else (row < last, row > 0)

        @pl.when(first)
        def _():
            pl.semaphore_wait(passed_on.at[int(upward)], 1)

        @pl.when(final)
        def _():
            to_dp(passed_on.at[int(upward)], me_d + 2 if upward else me_d - 2)

    def meet_half(which):
        for low_half in (True, False):
            @pl.when((row < rows_y // 2) if low_half else (row >= rows_y // 2))
            def _():
                scan(low_half == (which == 0))

    def send_slab(peer, src, dst, n):
        pltpu.make_async_remote_copy(
            src_ref=src.at[:, peer], dst_ref=dst.at[:, me_s],
            send_sem=send_sem.at[n], recv_sem=recv_sem.at[n],
            device_id={"slab": peer}, device_id_type=MESH,
        ).start()

    def send_earlier(src, dst, n):
        send_slab(partner, src, dst, n)
        for level in range(levels - 1):
            @pl.when(level < mine)
            def _():
                for half in range(2):
                    send_slab(half * 8 + level, src, dst, n)

    def exchange(axis, me, peers, src, dst, n, rank=0):
        lead = (slice(None),) * rank
        for peer in peers:
            pltpu.make_async_remote_copy(
                src_ref=src.at[(*lead, peer)], dst_ref=dst.at[(*lead, me)],
                send_sem=send_sem.at[n], recv_sem=recv_sem.at[n],
                device_id={axis: peer}, device_id_type=MESH,
            ).start()

    def wait_all(ref, count, sem):
        part = ref.at[pl.ds(0, count - 1)] if ref.shape[0] == count else ref.at[:, pl.ds(0, count - 1)]
        pltpu.make_async_copy(part, part, sem).wait()


    def over_slab(src, dst, n):
        for off in RING[:-1]:
            for half in range(2):
                send_slab(half * 8 + lax.rem(mine + off, 8), src, dst, n)
        send_slab(partner, src, dst, n)

    over_dp = functools.partial(exchange, "dp", me_d, peers_d)

    def along_y(field, send, h):
        for c in range(4):
            part = field[h * 128 + c * 32 : h * 128 + (c + 1) * 32].astype(F32).reshape(256, 256)
            for half in range(2):
                lines[half, c * 256 : (c + 1) * 256, :] = part[:, half * 128 : half * 128 + 128]
        for r in range(8):
            rows = jnp.concatenate(
                [lines[half, pl.ds(r, 128, stride=8), :] for half in range(2)], axis=1
            ).astype(BF16)
            folded[pl.ds(r, 64, stride=8), :] = nt(ty_ref[...], rows)
        send[h] = folded[...].astype(BF16).reshape(slabs, 2, 16, 128)

    loads[0].wait()
    loads[1].wait()
    along_y(cot_v, send_c, 0)
    loads[2].wait()
    along_y(cot_v, send_c, 1)
    send_earlier(send_c, got_c, 0)
    for h in range(2):
        got_c[h, me_s] = send_c[h, me_s]
    loads[3].wait()
    along_y(act_v, send_a, 0)
    along_y(act_v, send_a, 1)
    send_earlier(send_a, got_a, 2)
    for h in range(2):
        got_a[h, me_s] = send_a[h, me_s]
    meet_four()
    for level in range(1, levels):
        @pl.when(mine < level)
        def _():
            pl.semaphore_wait(ready.at[level], 2)
            for half in range(2):
                send_slab(half * 8 + level, send_c, got_c, 0)
            for half in range(2):
                send_slab(half * 8 + level, send_a, got_a, 2)

    pl.semaphore_wait(four, 2)
    meet_half(0)
    loads[4].wait()
    for c in range(8):
        part = w_v[c * 8 : (c + 1) * 8].astype(F32).reshape(512, 128)
        lines[c // 4, c % 4 * 512 : (c % 4 + 1) * 512, :] = part

    @pl.loop(0, 64)
    def _(m):
        for half in range(2):
            wm[m, half * 32 : half * 32 + 32, :] = lines[
                half, pl.ds(m, 32, stride=64), :
            ].astype(BF16)

    lane = lax.broadcasted_iota(jnp.int32, (32, 128), 1)
    low = lane < 64

    def spec_of(got):
        return [
            [
                jnp.dot(fx_ref[...], got[h, :, t].reshape(256, 128), preferred_element_type=F32)
                .astype(BF16)
                .astype(F32)
                for h in range(2)
            ]
            for t in range(2)
        ]

    def to_pair(specs, pair):
        for t in range(2):
            for q in range(2):
                for h in range(2):
                    spectra[pl.ds(t * 128 + q * 2 + h, 32, stride=4), :] = specs[t][h][
                        q * 32 : q * 32 + 32
                    ]
        pair[...] = spectra[...].astype(BF16).reshape(groups, 256 // groups, 128)

    meet_half(1)
    wait_all(got_c, slabs, recv_sem.at[0])
    loads[5].wait()
    loads[6].wait()
    specs = spec_of(got_c)

    for t in range(2):
        for h in range(2):
            re, im = specs[t][h][0:32], specs[t][h][32:64]
            re_r = pltpu.roll(re, 64, 1)
            im_r = pltpu.roll(im, 64, 1)
            rows = (
                jnp.where(low, re, im_r),
                jnp.where(low, im, -re_r),
                jnp.where(low, re_r, im),
                jnp.where(low, im_r, -re),
            )
            for n, row in enumerate(rows):
                stacked[pl.ds(t * 256 + h * 4 + n, 32, stride=8), :] = row

    for n in range(16):
        both = nt(
            stacked[n * 32 : n * 32 + 32, :].astype(BF16),
            wm[n * 4 : n * 4 + 4].reshape(256, 128),
        )
        for m in range(4):
            block = both[m * 8 : m * 8 + 8, m // 2 * 128 : m // 2 * 128 + 128]
            mixed[n * 32 + m * 8 : n * 32 + m * 8 + 8, :] = (
                pltpu.roll(block, 64, 1) if m % 2 else block
            )

    for t in range(2):
        rows = []
        for q in range(2):
            tiles = []
            for h in range(2):
                first = mixed[pl.ds(t * 256 + h * 4 + q, 32, stride=8), :]
                second = mixed[pl.ds(t * 256 + h * 4 + 2 + q, 32, stride=8), :]
                tiles.append(jnp.where(low, first, pltpu.roll(second, 64, 1)))
            rows.append(jnp.concatenate(tiles, axis=1))
        grads = jnp.concatenate(rows, axis=0).astype(BF16)
        spread = jnp.dot(tx_ref[:, 0:64], grads, preferred_element_type=F32)
        for h in range(2):
            send_e[h, :, t] = (
                spread[:, h * 128 : h * 128 + 128].astype(BF16).reshape(slabs, 16, 128)
            )
    for h in range(2):
        got_e[h, me_s] = send_e[h, me_s]

    to_pair(specs, pair_c)
    all_c[me_d] = pair_c[me_d]
    over_dp(pair_c, all_c, 4)

    wait_all(got_a, slabs, recv_sem.at[2])
    over_slab(send_e, got_e, 3)
    to_pair(spec_of(got_a), pair_a)
    all_a[me_d] = pair_a[me_d]
    over_dp(pair_a, all_a, 5)

    wait_all(all_c, groups, recv_sem.at[4])
    wait_all(all_a, groups, recv_sem.at[5])
    sums[0] = all_a[...].astype(F32).reshape(256, 128)
    sums[1] = all_c[...].astype(F32).reshape(256, 128)
    wide = lax.broadcasted_iota(jnp.int32, (64, 128), 1) < 64
    for m in range(2):
        def part(which, q):
            return jnp.concatenate(
                [sums[which, pl.ds(m * 4 + q * 2 + h, groups, stride=8), :] for h in range(2)],
                axis=0,
            )

        ins = jnp.concatenate([part(0, 0), part(0, 1)], axis=0).astype(BF16)
        out_re, out_im = part(1, 0), part(1, 1)
        outs = jnp.concatenate([out_re, out_im], axis=0)
        swapped = jnp.concatenate([out_im, -out_re], axis=0)
        prod = tn(ins, jnp.concatenate([outs, swapped], axis=1).astype(BF16))
        top, bottom = prod[0:64], prod[64:128]
        total = jnp.where(
            wide,
            top[:, 0:128] + pltpu.roll(bottom[:, 0:128], 64, 1),
            pltpu.roll(top[:, 128:256], 64, 1) + bottom[:, 128:256],
        )
        mixed[m * 64 : m * 64 + 64, :] = total
    for m in range(2):
        for i in range(2):
            wsend[i, :, m, :] = mixed[pl.ds(m * 64 + i, groups, stride=2), :]
    for i in range(2):
        wgrad_ref[i, me_d] = wsend[i, me_d]
    over_dp(wsend, wgrad_ref, 6, rank=1)

    wait_all(got_e, slabs, recv_sem.at[3])
    for h in range(2):
        folded[...] = got_e[h].astype(F32).reshape(512, 128)
        for r in range(8):
            values = tn(folded[pl.ds(r, 64, stride=8), :].astype(BF16), ty_ref[...])
            for half in range(2):
                lines[half, pl.ds(r, 128, stride=8), :] = values[
                    :, half * 128 : half * 128 + 128
                ]
        for c in range(4):
            grad_ref[h * 128 + c * 32 : h * 128 + (c + 1) * 32] = (
                jnp.concatenate(
                    [lines[half, c * 256 : (c + 1) * 256, :] for half in range(2)], axis=1
                )
                .astype(BF16)
                .reshape(32, 8, 256)
            )
    wait_all(wgrad_ref, groups, recv_sem.at[6])
    for n, ref in ((0, send_c), (2, send_a), (3, send_e)):
        wait_all(ref, slabs, send_sem.at[n])
    for n, ref in enumerate((pair_c, pair_a, wsend)):
        wait_all(ref, groups, send_sem.at[4 + n])


def write_out(grad_ref, wgrad_ref, grad_hbm, wgrad_hbm, sems):
    copies = [
        pltpu.make_async_copy(grad_ref, grad_hbm, sems.at[0]),
        pltpu.make_async_copy(wgrad_ref, wgrad_hbm, sems.at[1]),
    ]
    for copy in copies:
        copy.start()
    for copy in copies:
        copy.wait()


def body(activation, cotangent, spectral_weight, slabs, groups):
    ty, packed = tables(slabs)
    block = (2, slabs, 2, 16, 128)
    pair = (groups, 256 // groups, 128)
    total = (2, groups, 2, 128)
    got, wgrad = pl.pallas_call(
        functools.partial(kernel, slabs, groups),
        out_shape=(
            jax.ShapeDtypeStruct((256, 8, 256), BF16),
            jax.ShapeDtypeStruct(total, F32),
        ),
        in_specs=[pl.BlockSpec(memory_space=pltpu.HBM)] * 4,
        out_specs=[pl.BlockSpec(memory_space=pltpu.VMEM)] * 2,
        scratch_shapes=[
            pltpu.VMEM((64, 256), BF16),
            pltpu.VMEM((64, 256), BF16),
            pltpu.VMEM((256, 128), BF16),
            pltpu.VMEM((256, 8, 256), BF16),
            pltpu.VMEM((256, 8, 256), BF16),
            pltpu.VMEM((64, 64, 128), BF16),
            pltpu.VMEM((64, 64, 128), BF16),
            pltpu.VMEM((2, 2048, 128), F32),
            pltpu.VMEM((512, 128), F32),
        ]
        + [pltpu.VMEM(block, BF16)] * 6
        + [pltpu.VMEM((256, 128), F32)]
        + [pltpu.VMEM(pair, BF16)] * 4
        + [
            pltpu.VMEM((512, 128), F32),
            pltpu.VMEM((512, 128), F32),
            pltpu.VMEM((2, 256, 128), F32),
            pltpu.VMEM(total, F32),
            pltpu.SemaphoreType.DMA((7,)),
            pltpu.SemaphoreType.DMA((7,)),
            pltpu.SemaphoreType.DMA((7,)),
            pltpu.SemaphoreType.REGULAR((slabs // 2,)),
            pltpu.SemaphoreType.REGULAR,
            pltpu.SemaphoreType.REGULAR,
            pltpu.SemaphoreType.REGULAR((2,)),
        ],
        compiler_params=pltpu.CompilerParams(
            collective_id=0, has_side_effects=True, vmem_limit_bytes=67043328 - 12200000
        ),
    )(
        activation.reshape(256, 8, 256),
        cotangent.reshape(256, 8, 256),
        spectral_weight.reshape(64, 64, 128),
        packed,
    )
    grad, wgrad = pl.pallas_call(
        write_out,
        out_shape=(jax.ShapeDtypeStruct((256, 8, 256), BF16), jax.ShapeDtypeStruct(total, F32)),
        in_specs=[pl.BlockSpec(memory_space=pltpu.VMEM)] * 2,
        out_specs=[pl.BlockSpec(memory_space=pltpu.HBM)] * 2,
        scratch_shapes=[pltpu.SemaphoreType.DMA((2,))],
        compiler_params=pltpu.CompilerParams(vmem_limit_bytes=20 << 20),
    )(got, wgrad)
    return grad.reshape(4, 64, 8, 256), wgrad.reshape(2, 2, 32, 128)


def solution(mesh):
    placed = (P("dp", None, "slab", None), P("dp", None, "slab", None), P(None, "slab", None, None))
    return jax.shard_map(
        functools.partial(body, slabs=mesh.shape["slab"], groups=mesh.shape["dp"]),
        mesh=mesh,
        in_specs=placed,
        out_specs=(P("dp", None, "slab", None), P("dp", "slab", None, None)),
        check_vma=False,
    )
```
